32 devices in a mesh: atoms: 8 (over z, x), modes: 4 (over y, core).
Axes of the slice: x: 2, y: 2, z: 4, core: 2. Of those that a mesh axis runs over, the one named last changes fastest.
Arguments:
- subspace: float32 [768, 16384], P('modes', 'atoms'), may hold values from -100 to 100
- applied: float32 [768, 16384], P('modes', 'atoms'), may hold values from -300 to 300
Outputs:
- ortho_basis: float32 [768, 16384], P('modes', 'atoms')
- projected: float32 [768, 768], P('modes')
The draws below stay inside these ranges and needn't reach their ends.
All inputs are finite; a program needn't handle non-finite values.
Results may differ from the reference program's by a relative error of at most 0.00025.
Values sent between devices are 32-bit elements; how exact they have to be, the bound alone decides.
No kernel may reach another device: no remote copies, remote signals or barrier semaphores. Data moves between devices by JAX's collectives and lax.ppermute only.
A program may use at most 64 MiB of HBM per device.

```python
import math
import jax
import jax.numpy as jnp
from jax import lax

K = 768
NROWS = 16384


def mixed_subspace(key):
    keys = jax.random.split(jax.random.fold_in(key, 11), 3)
    normals = jax.random.truncated_normal(keys[0], -6.0, 6.0, (NROWS, K), jnp.float32)
    weights = jax.random.truncated_normal(keys[1], -4.0, 4.0, (K, K), jnp.float32)
    mixing = jnp.eye(K, dtype=jnp.float32) + 0.5 * weights / math.sqrt(K)
    col_scale = jnp.exp(jax.random.uniform(keys[2], (K,), jnp.float32, 0.0, math.log(10.0)))
    mixed = jnp.dot(normals, mixing, precision=lax.Precision.HIGHEST)
    return jnp.clip(mixed * col_scale[None, :], -100.0, 100.0)


def draw_subspace(key, part):
    return mixed_subspace(key).T


def draw_applied(key, part):
    vectors = mixed_subspace(key)
    keys = jax.random.split(jax.random.fold_in(key, 23), 3)
    eigen_part = jax.random.uniform(keys[0], (K,), jnp.float32, -1.0, 2.0)
    weights = jax.random.truncated_normal(keys[1], -4.0, 4.0, (K, K), jnp.float32)
    coupling = jnp.diag(eigen_part) + 0.3 * (weights + weights.T) / math.sqrt(2.0 * K)
    jitter = jax.random.truncated_normal(keys[2], -6.0, 6.0, (NROWS, K), jnp.float32)
    result = jnp.dot(vectors, coupling, precision=lax.Precision.HIGHEST) + 2.0 * jitter
    return jnp.clip(result, -300.0, 300.0).T


def setup_inputs(seed: int = 0) -> dict:
    key_list = jax.random.split(jax.random.key(seed), 3)
    return {
        "subspace": draw_subspace(jax.random.fold_in(key_list[2], 71), 0),
        "applied": draw_applied(jax.random.fold_in(key_list[2], 71), 0),
    }


def reference(subspace, applied):
    highest = lax.Precision.HIGHEST
    gram = jnp.dot(subspace.astype(jnp.float32), subspace.T.astype(jnp.float32), precision=highest, preferred_element_type=jnp.float32) / NROWS
    cross = jnp.dot(subspace.astype(jnp.float32), applied.T.astype(jnp.float32), precision=highest, preferred_element_type=jnp.float32) / NROWS
    factor = jnp.linalg.cholesky(gram)
    identity = jnp.eye(K, dtype=gram.dtype)
    inv_lower = lax.linalg.triangular_solve(factor, identity, left_side=True, lower=True)
    inv_upper = inv_lower.T
    ortho_basis = jnp.dot(inv_lower.astype(jnp.float32), subspace.astype(jnp.float32), precision=highest, preferred_element_type=jnp.float32)
    half_proj = jnp.dot(inv_lower.astype(jnp.float32), cross.astype(jnp.float32), precision=highest, preferred_element_type=jnp.float32)
    projected = jnp.dot(half_proj.astype(jnp.float32), inv_upper.astype(jnp.float32), precision=highest, preferred_element_type=jnp.float32)
    return (ortho_basis, projected)
```

```python
import jax
import jax.numpy as jnp
from jax import lax
from jax.experimental import pallas as pl
from jax.experimental.pallas import tpu as pltpu
from jax.sharding import PartitionSpec as P

LANES = 128
SUB = 32
PREC = lax.Precision.HIGHEST


def mm(a, b, prec=None):
    return lax.dot_general(a, b, (((1,), (0,)), ((), ())), precision=prec or PREC, preferred_element_type=jnp.float32)


def base_factor(w, s):
    lane = lax.broadcasted_iota(jnp.int32, (SUB, LANES), 1)
    row = lax.broadcasted_iota(jnp.int32, (SUB, LANES), 0)
    cols = [jnp.broadcast_to(w[:, SUB * s + k : SUB * s + k + 1], (SUB, LANES)) for k in range(SUB)]
    in_block = (lane >= SUB * s) & (lane < SUB * (s + 1))
    w = jnp.where(in_block, (lane - SUB * s == row).astype(jnp.float32), w)
    scale = jnp.ones((SUB, LANES), jnp.float32)
    for k in range(SUB):
        g = (k // 8) * 8
        r = k - g
        rows = SUB - g
        live = row[:rows] > r
        pivot = jnp.broadcast_to(cols[k][r : r + 1], (rows, LANES))
        scale_new = lax.rsqrt(pivot)
        inv = 1.0 / pivot[:8]
        inv = jnp.broadcast_to(inv[:1], (rows, LANES)) if rows > 8 else inv
        c = jnp.where(live, cols[k] * inv, 0.0)
        scale = jnp.concatenate([scale[:g], jnp.where(row[:rows] == r, scale_new, scale[g:])], 0) if g else jnp.where(row == r, scale_new, scale)
        drop = 8 if r == 7 else 0
        for m in range(k + 1, SUB):
            cols[m] = (cols[m] - c * jnp.broadcast_to(cols[m][r : r + 1], (rows, LANES)))[drop:]
        tail = w[g:] - c * jnp.broadcast_to(w[k : k + 1], (rows, LANES))
        w = jnp.concatenate([w[:g], tail], 0) if g else tail
    return w * scale


def diag_factor(a):
    n = LANES // SUB
    blocks = [a[SUB * t : SUB * (t + 1)] for t in range(n)]
    lane = lax.broadcasted_iota(jnp.int32, (SUB, LANES), 1)
    for s in range(n):
        blocks[s] = base_factor(blocks[s], s)
        if s + 1 < n:
            coef = jnp.transpose(blocks[s])[SUB * (s + 1) :]
            delta = mm(coef, blocks[s])
            keep = (lane < SUB * s) | (lane >= SUB * (s + 1))
            for t in range(s + 1, n):
                blocks[t] = jnp.where(keep, blocks[t], 0.0) - delta[SUB * (t - s - 1) : SUB * (t - s)]
    full = jnp.concatenate(blocks, 0)
    r = lax.broadcasted_iota(jnp.int32, (LANES, LANES), 0)
    c = lax.broadcasted_iota(jnp.int32, (LANES, LANES), 1)
    return jnp.where(c <= r, full, 0.0)


def inverse_kernel(g_ref, x_ref):
    size = g_ref.shape[0]
    n = size // LANES
    x_ref[...] = g_ref[...]

    def at(t):
        return pl.ds(pl.multiple_of(t * LANES, LANES), LANES)

    def step(p, _):
        x = diag_factor(x_ref[at(p), at(p)])
        panel = mm(x, x_ref[at(p), :])
        x_ref[at(p), :] = panel
        x_ref[at(p), at(p)] = x

        def trailing(t, _):
            coef = jnp.transpose(x_ref[at(p), at(t)])
            x_ref[at(t), at(p)] = jnp.zeros((LANES, LANES), jnp.float32)
            x_ref[at(t), :] = x_ref[at(t), :] - mm(coef, x_ref[at(p), :])
            return 0

        lax.fori_loop(p + 1, n, trailing, 0)
        return 0

    lax.fori_loop(0, n, step, 0)
    for t in range(n - 1):
        x_ref[LANES * t : LANES * (t + 1), LANES * (t + 1) :] = jnp.zeros((LANES, size - LANES * (t + 1)), jnp.float32)


def cholesky_inverse(gram):
    return pl.pallas_call(
        inverse_kernel,
        out_shape=jax.ShapeDtypeStruct(gram.shape, jnp.float32),
        in_specs=[pl.BlockSpec(memory_space=pltpu.VMEM)],
        out_specs=pl.BlockSpec(memory_space=pltpu.VMEM),
        cost_estimate=pl.CostEstimate(flops=50_000_000_000, bytes_accessed=4_000_000, transcendentals=0),
    )(gram)


def contract_cols(left, right):
    return lax.dot_general(
        left, right, (((1,), (1,)), ((), ())), precision=lax.Precision.HIGH, preferred_element_type=jnp.float32
    )


def per_device(subspace, applied):
    mode_width = subspace.shape[0]
    row_total = subspace.shape[1] * lax.axis_size("atoms")
    mode_start = lax.axis_index("modes") * mode_width
    full_modes = lax.all_gather(subspace, "modes", axis=0, tiled=True)
    gram_part = contract_cols(subspace, full_modes) / row_total
    crosst_part = contract_cols(applied, full_modes) / row_total
    gram_rows, crosst_rows = lax.psum((gram_part, crosst_part), "atoms")
    gram_full = lax.all_gather(gram_rows, "modes", axis=0, tiled=True)
    crosst_full = lax.all_gather(crosst_rows, "modes", axis=0, tiled=True)
    inv_lower = cholesky_inverse(gram_full)
    lower_rows = lax.dynamic_slice_in_dim(inv_lower, mode_start, mode_width, 0)
    high = lax.Precision.HIGH
    ortho_basis = mm(lower_rows, full_modes, high)
    projected = contract_cols(contract_cols(lower_rows, crosst_full), inv_lower)
    return (ortho_basis, projected)


def solution(mesh):
    return jax.shard_map(
        per_device,
        mesh=mesh,
        in_specs=(P("modes", "atoms"), P("modes", "atoms")),
        out_specs=(P("modes", "atoms"), P("modes", None)),
        check_vma=False,
    )
```

```python
import functools

import jax
import jax.numpy as jnp
from jax import lax
from jax.experimental import pallas as pl
from jax.experimental.pallas import tpu as pltpu
from jax.sharding import PartitionSpec as P

HIGH = lax.Precision.HIGH
VMEM = pl.BlockSpec(memory_space=pltpu.VMEM)
ANY = pl.BlockSpec(memory_space=pl.ANY)

LANES = 128
SUB = 32
PREC = lax.Precision.HIGHEST


def mm(a, b, prec=None):
    return lax.dot_general(a, b, (((1,), (0,)), ((), ())), precision=prec or PREC, preferred_element_type=jnp.float32)


def base_factor(w, s):
    lane = lax.broadcasted_iota(jnp.int32, (SUB, LANES), 1)
    row = lax.broadcasted_iota(jnp.int32, (SUB, LANES), 0)
    cols = [jnp.broadcast_to(w[:, SUB * s + k : SUB * s + k + 1], (SUB, LANES)) for k in range(SUB)]
    in_block = (lane >= SUB * s) & (lane < SUB * (s + 1))
    w = jnp.where(in_block, (lane - SUB * s == row).astype(jnp.float32), w)
    scale = jnp.ones((SUB, LANES), jnp.float32)
    for k in range(SUB):
        g = (k // 8) * 8
        r = k - g
        rows = SUB - g
        live = row[:rows] > r
        pivot = jnp.broadcast_to(cols[k][r : r + 1], (rows, LANES))
        scale_new = lax.rsqrt(pivot)
        inv = 1.0 / pivot[:8]
        inv = jnp.broadcast_to(inv[:1], (rows, LANES)) if rows > 8 else inv
        c = jnp.where(live, cols[k] * inv, 0.0)
        scale = jnp.concatenate([scale[:g], jnp.where(row[:rows] == r, scale_new, scale[g:])], 0) if g else jnp.where(row == r, scale_new, scale)
        drop = 8 if r == 7 else 0
        for m in range(k + 1, SUB):
            cols[m] = (cols[m] - c * jnp.broadcast_to(cols[m][r : r + 1], (rows, LANES)))[drop:]
        tail = w[g:] - c * jnp.broadcast_to(w[k : k + 1], (rows, LANES))
        w = jnp.concatenate([w[:g], tail], 0) if g else tail
    return w * scale


def diag_factor(a):
    n = LANES // SUB
    blocks = [a[SUB * t : SUB * (t + 1)] for t in range(n)]
    lane = lax.broadcasted_iota(jnp.int32, (SUB, LANES), 1)
    for s in range(n):
        blocks[s] = base_factor(blocks[s], s)
        if s + 1 < n:
            coef = jnp.transpose(blocks[s])[SUB * (s + 1) :]
            delta = mm(coef, blocks[s])
            keep = (lane < SUB * s) | (lane >= SUB * (s + 1))
            for t in range(s + 1, n):
                blocks[t] = jnp.where(keep, blocks[t], 0.0) - delta[SUB * (t - s - 1) : SUB * (t - s)]
    full = jnp.concatenate(blocks, 0)
    r = lax.broadcasted_iota(jnp.int32, (LANES, LANES), 0)
    c = lax.broadcasted_iota(jnp.int32, (LANES, LANES), 1)
    return jnp.where(c <= r, full, 0.0)


def nt(a, b, prec=HIGH):
    return lax.dot_general(a, b, (((1,), (1,)), ((), ())), precision=prec, preferred_element_type=jnp.float32)


def bits(axis):
    return range(lax.axis_size(axis).bit_length() - 1)


def swap(x, axis, bit):
    return lax.ppermute(x, axis, [(i, i ^ (1 << bit)) for i in range(lax.axis_size(axis))])


def side(axis, bit):
    return (lax.axis_index(axis) >> bit) & 1


def reduce_scatter_bit(x, axis, bit):
    half = x.shape[0] // 2
    b = side(axis, bit)
    send = lax.dynamic_slice_in_dim(x, (1 - b) * half, half, 0)
    return lax.dynamic_slice_in_dim(x, b * half, half, 0) + swap(send, axis, bit)


def all_gather_bit(x, axis, bit):
    other = swap(x, axis, bit)
    first = side(axis, bit) == 0
    return jnp.concatenate([jnp.where(first, x, other), jnp.where(first, other, x)], 0)


def all_reduce_atoms(x):
    order = list(bits("atoms"))
    scattered = []
    for b in order:
        if b != order[-1] and x.shape[0] % 16 == 0:
            x = reduce_scatter_bit(x, "atoms", b)
            scattered.append(b)
        else:
            x = x + swap(x, "atoms", b)
    for b in reversed(scattered):
        x = all_gather_bit(x, "atoms", b)
    return x


def all_gather_modes(x):
    shape = x.shape
    x = x[None]
    for b in reversed(bits("modes")):
        other = swap(x, "modes", b)
        first = side("modes", b) == 0
        x = jnp.stack([jnp.where(first, x, other), jnp.where(first, other, x)], 1).reshape((-1,) + shape)
    return x.reshape(-1, shape[1])


def gather_pieces(x):
    width = x.shape[1]
    half = width // 2
    out = []
    for start in (0, half):
        part = x[:, start : start + half]
        held = [(0, part)]
        for b in reversed(bits("modes")):
            held += [(mask ^ (1 << b), swap(piece, "modes", b)) for mask, piece in held]
        out += [(mask, start, piece) for mask, piece in held]
    return out


def load_pieces(meta, index_ref, refs, scratch, sem):
    rows = refs[0].shape[0]
    copies = []
    for i, ((mask, start), ref) in enumerate(zip(meta, refs)):
        row = pl.multiple_of((index_ref[0] ^ mask) * rows, 8)
        copies.append(
            pltpu.make_async_copy(ref, scratch.at[pl.ds(row, rows), pl.ds(start, ref.shape[1])], sem.at[i])
        )
    for copy in copies:
        copy.start()
    return copies


def gram_kernel(meta, total, index_ref, blocks_ref, *refs):
    pieces, (out_ref, scratch, sem) = refs[: len(meta)], refs[len(meta) :]
    for copy in load_pieces(meta, index_ref, pieces, scratch, sem):
        copy.wait()
    count = out_ref.shape[0] // LANES
    depth = scratch.shape[1]
    chunk = min(512, depth)

    def block(i, _):
        p = pl.multiple_of(blocks_ref[0, i] * LANES, LANES)
        t = pl.multiple_of(blocks_ref[1, i] * LANES, LANES)
        acc = jnp.zeros((LANES, LANES), jnp.float32)
        for k in range(0, depth, chunk):
            acc += nt(scratch[pl.ds(p, LANES), k : k + chunk], scratch[pl.ds(t, LANES), k : k + chunk])
        out_ref[pl.ds(pl.multiple_of(i * LANES, LANES), LANES), :] = acc / total
        return 0

    lax.fori_loop(0, count, block, 0)


def cross_kernel(meta, total, index_ref, applied_ref, *refs):
    pieces, (out_ref, scratch, sem) = refs[: len(meta)], refs[len(meta) :]
    for copy in load_pieces(meta, index_ref, pieces, scratch, sem):
        copy.wait()
    depth = scratch.shape[1]
    chunk = min(512, depth)
    wide = 2 * LANES

    def block(i, _):
        at = pl.multiple_of(i * wide, wide)
        acc = jnp.zeros((out_ref.shape[0], wide), jnp.float32)
        for k in range(0, depth, chunk):
            acc += nt(applied_ref[:, k : k + chunk], scratch[pl.ds(at, wide), k : k + chunk])
        out_ref[:, pl.ds(at, wide)] = acc / total
        return 0

    lax.fori_loop(0, out_ref.shape[1] // wide, block, 0)


def final_kernel(meta, index_ref, inv_ref, crosst_ref, *refs):
    pieces, (ortho_ref, proj_ref, scratch, sem) = refs[: len(meta)], refs[len(meta) :]
    copies = load_pieces(meta, index_ref, pieces, scratch, sem)
    rows = ortho_ref.shape[0]
    mine = pl.ds(pl.multiple_of(index_ref[0] * rows, 8), rows)
    half = nt(inv_ref[mine, :], crosst_ref[...])
    proj_ref[...] = nt(half, inv_ref[...])
    for copy in copies:
        copy.wait()
    chunk = min(512, ortho_ref.shape[1])

    def block(i, _):
        at = pl.multiple_of(i * chunk, chunk)
        ortho_ref[:, pl.ds(at, chunk)] = mm(inv_ref[mine, :], scratch[:, pl.ds(at, chunk)], HIGH)
        return 0

    lax.fori_loop(0, ortho_ref.shape[1] // chunk, block, 0)


def cost(flops, moved):
    return pl.CostEstimate(flops=int(flops), bytes_accessed=int(moved), transcendentals=0)


def inverse_kernel(n, packed_ref, x_ref):
    size = x_ref.shape[0]
    i = 0
    for p in range(n):
        for t in range(n):
            spot = (slice(LANES * p, LANES * (p + 1)), slice(LANES * t, LANES * (t + 1)))
            if t >= p:
                x_ref[spot] = packed_ref[LANES * i : LANES * (i + 1), :]
                i += 1
            else:
                x_ref[spot] = jnp.zeros((LANES, LANES), jnp.float32)

    def at(t):
        return pl.ds(pl.multiple_of(t * LANES, LANES), LANES)

    def step(p, _):
        x = diag_factor(x_ref[at(p), at(p)])
        panel = mm(x, x_ref[at(p), :])
        x_ref[at(p), :] = panel
        x_ref[at(p), at(p)] = x

        def trailing(t, _):
            coef = jnp.transpose(x_ref[at(p), at(t)])
            x_ref[at(t), at(p)] = jnp.zeros((LANES, LANES), jnp.float32)
            x_ref[at(t), :] = x_ref[at(t), :] - mm(coef, x_ref[at(p), :])
            return 0

        lax.fori_loop(p + 1, n, trailing, 0)
        return 0

    lax.fori_loop(0, n, step, 0)
    for t in range(n - 1):
        x_ref[LANES * t : LANES * (t + 1), LANES * (t + 1) :] = jnp.zeros((LANES, size - LANES * (t + 1)), jnp.float32)


def per_device(subspace, applied):
    width, depth = subspace.shape
    size = width * lax.axis_size("modes")
    total = depth * lax.axis_size("atoms")
    panels = size // LANES
    upper = [(p, t) for p in range(panels) for t in range(p, panels)]
    per = -(-len(upper) // lax.axis_size("modes"))
    table = jnp.array((upper + upper[-1:] * (per * lax.axis_size("modes") - len(upper))), jnp.int32).T
    index = lax.axis_index("modes")
    mine = lax.dynamic_slice_in_dim(table, index * per, per, 1)
    index = index[None]

    found = gather_pieces(subspace)
    meta = tuple((mask, start) for mask, start, _ in found)
    pieces = [piece for _, _, piece in found]
    smem = pl.BlockSpec(memory_space=pltpu.SMEM)
    scratch = [pltpu.VMEM((size, depth), jnp.float32), pltpu.SemaphoreType.DMA((len(pieces),))]

    gram = pl.pallas_call(
        functools.partial(gram_kernel, meta, float(total)),
        out_shape=jax.ShapeDtypeStruct((per * LANES, LANES), jnp.float32),
        in_specs=[smem, smem] + [ANY] * len(pieces),
        out_specs=VMEM,
        scratch_shapes=scratch,
        cost_estimate=cost(2e9, 8e6),
        name="gram",
    )(index, mine, *pieces)
    gram = all_reduce_atoms(gram)
    gram = all_gather_modes(gram)

    crosst = pl.pallas_call(
        functools.partial(cross_kernel, meta, float(total)),
        out_shape=jax.ShapeDtypeStruct((width, size), jnp.float32),
        in_specs=[smem, VMEM] + [ANY] * len(pieces),
        out_specs=VMEM,
        scratch_shapes=scratch,
        cost_estimate=cost(4e9, 8e6),
        name="cross",
    )(index, applied, *pieces)
    crosst = all_reduce_atoms(crosst)
    crosst = all_gather_modes(crosst)

    inv_lower = pl.pallas_call(
        functools.partial(inverse_kernel, panels),
        out_shape=jax.ShapeDtypeStruct((size, size), jnp.float32),
        in_specs=[VMEM],
        out_specs=VMEM,
        cost_estimate=cost(20e9, 4e6),
        name="inverse",
    )(gram)
    return pl.pallas_call(
        functools.partial(final_kernel, meta),
        out_shape=(
            jax.ShapeDtypeStruct((width, depth), jnp.float32),
            jax.ShapeDtypeStruct((width, size), jnp.float32),
        ),
        in_specs=[smem, VMEM, VMEM] + [ANY] * len(pieces),
        out_specs=(VMEM, VMEM),
        scratch_shapes=scratch,
        cost_estimate=cost(4e9, 8e6),
        name="final",
    )(index, inv_lower, crosst, *pieces)


def solution(mesh):
    return jax.shard_map(
        per_device,
        mesh=mesh,
        in_specs=(P("modes", "atoms"), P("modes", "atoms")),
        out_specs=(P("modes", "atoms"), P("modes", None)),
        check_vma=False,
    )
```

```python
import functools

import jax
import jax.numpy as jnp
from jax import lax
from jax.experimental import pallas as pl
from jax.experimental.pallas import tpu as pltpu
from jax.sharding import PartitionSpec as P


HIGH = lax.Precision.HIGH
VMEM = pl.BlockSpec(memory_space=pltpu.VMEM)
ANY = pl.BlockSpec(memory_space=pl.ANY)

LANES = 128
SUB = 32
PREC = lax.Precision.HIGHEST


def mm(a, b, prec=None):
    return lax.dot_general(a, b, (((1,), (0,)), ((), ())), precision=prec or PREC, preferred_element_type=jnp.float32)


def base_factor(w, s):
    lane = lax.broadcasted_iota(jnp.int32, (SUB, LANES), 1)
    row = lax.broadcasted_iota(jnp.int32, (SUB, LANES), 0)
    sub = lax.broadcasted_iota(jnp.int32, (8, LANES), 0)

    def column(rows, k):
        return [jnp.broadcast_to(r[:, SUB * s + k : SUB * s + k + 1], (8, LANES)) for r in rows]

    def one(tile, r):
        return jnp.broadcast_to(tile[r : r + 1], (8, LANES))

    groups = SUB // 8
    first = [w[8 * g : 8 * (g + 1)] for g in range(groups)]
    in_block = (lane >= SUB * s) & (lane < SUB * (s + 1))
    own = jnp.where(in_block, (lane - SUB * s == row).astype(jnp.float32), w)
    held = [own[8 * g : 8 * (g + 1)] for g in range(groups)]
    raw = list(first)
    ahead = SUB // 2
    cols = {m: column(first[m // 8 :], m) for m in range(ahead)}
    scales = [jnp.ones((8, LANES), jnp.float32) for _ in range(groups)]
    for k in range(SUB):
        g, r = divmod(k, 8)
        if k == 8:
            for m in range(ahead, SUB):
                cols[m] = column(raw[m // 8 :], m)
        mine = cols.pop(k)
        pivot = one(mine[0], r)
        scales[g] = jnp.where(sub == r, lax.rsqrt(pivot), scales[g])
        inv = 1.0 / pivot
        mult = [t * inv for t in mine]
        mult[0] = jnp.where(sub > r, mult[0], 0.0)
        for m, tiles in cols.items():
            across = one(mine[m // 8 - g], m % 8)
            cols[m] = [t - mult[i + m // 8 - g] * across for i, t in enumerate(tiles)]
        base = one(held[g], r)
        if k < 8:
            across = one(raw[g], r)
            for i in range(g, groups):
                raw[i] = raw[i] - mult[i - g] * across
        for i in range(g, groups):
            held[i] = held[i] - mult[i - g] * base
    return jnp.concatenate([h * c for h, c in zip(held, scales)], 0)


def diag_factor(a):
    n = LANES // SUB
    blocks = [a[SUB * t : SUB * (t + 1)] for t in range(n)]
    lane = lax.broadcasted_iota(jnp.int32, (SUB, LANES), 1)
    for s in range(n):
        blocks[s] = base_factor(blocks[s], s)
        if s + 1 < n:
            coef = jnp.transpose(blocks[s])[SUB * (s + 1) :]
            delta = mm(coef, blocks[s])
            keep = (lane < SUB * s) | (lane >= SUB * (s + 1))
            for t in range(s + 1, n):
                blocks[t] = jnp.where(keep, blocks[t], 0.0) - delta[SUB * (t - s - 1) : SUB * (t - s)]
    full = jnp.concatenate(blocks, 0)
    r = lax.broadcasted_iota(jnp.int32, (LANES, LANES), 0)
    c = lax.broadcasted_iota(jnp.int32, (LANES, LANES), 1)
    return jnp.where(c <= r, full, 0.0)


def nt(a, b, prec=HIGH):
    return lax.dot_general(a, b, (((1,), (1,)), ((), ())), precision=prec, preferred_element_type=jnp.float32)


def bits(axis):
    return range(lax.axis_size(axis).bit_length() - 1)


def swap(x, axis, bit):
    return lax.ppermute(x, axis, [(i, i ^ (1 << bit)) for i in range(lax.axis_size(axis))])


def side(axis, bit):
    return (lax.axis_index(axis) >> bit) & 1


def reduce_scatter_bit(x, axis, bit):
    half = x.shape[0] // 2
    b = side(axis, bit)
    send = lax.dynamic_slice_in_dim(x, (1 - b) * half, half, 0)
    got = swap(send, axis, bit)
    return lax.dynamic_slice_in_dim(x, b * half, half, 0) + got


def all_gather_bit(x, axis, bit):
    other = swap(x, axis, bit)
    first = side(axis, bit) == 0
    return jnp.concatenate([jnp.where(first, x, other), jnp.where(first, other, x)], 0)


def all_reduce_atoms(x):
    order = list(bits("atoms"))
    scattered = []
    for b in order:
        if b != order[-1] and x.shape[0] % 16 == 0:
            x = reduce_scatter_bit(x, "atoms", b)
            scattered.append(b)
        else:
            got = swap(x, "atoms", b)
            x = x + got
    for b in reversed(scattered):
        x = all_gather_bit(x, "atoms", b)
    return x


def gather_modes_pair(x):
    shape = x.shape
    x = x[None]
    for b in reversed(bits("modes")):
        other = swap(x, "modes", b)
        if b == 0:
            return x, other
        first = side("modes", b) == 0
        x = jnp.stack([jnp.where(first, x, other), jnp.where(first, other, x)], 1).reshape((-1,) + shape)


def pick(pair, core, mode, rows):
    mine, other = pair
    group, which = divmod(mode, 2)
    return jnp.where(core == which, mine[group, rows, :], other[group, rows, :])


def load_pieces(index_ref, keep, pieces, lo, scratch, sem):
    copies = []
    hi = lo + scratch.shape[1]
    for (mask, start), ref in pieces:
        rows = ref.shape[0]
        row = pl.multiple_of(((index_ref[0] ^ mask) & keep) * rows, 8)
        left, right = max(lo, start), min(hi, start + ref.shape[1])
        if left < right:
            source = ref.at[:, pl.ds(left - start, right - left)]
            target = scratch.at[pl.ds(row, rows), pl.ds(left - lo, right - left)]
            copies.append(pltpu.make_async_copy(source, target, sem.at[len(copies)]))
    for copy in copies:
        copy.start()
    return copies


def products_kernel(meta, keep, lo, total, with_sum, index_ref, blocks_ref, base_ref, applied_ref, *refs):
    sums, refs = (refs[:1], refs[1:]) if with_sum else ((), refs)
    pieces, (out_ref, scratch, sem) = refs[: len(meta)], refs[len(meta) :]
    for copy in load_pieces(index_ref, keep, list(zip(meta, pieces)), lo, scratch, sem):
        copy.wait()
    depth = scratch.shape[1]
    chunk = min(512, depth)
    width = applied_ref.shape[0]
    count = blocks_ref.shape[1]

    def store(at, acc):
        acc = acc / total
        out_ref[at, :] = acc + sums[0][at, :] if with_sum else acc

    def block(i, _):
        p = pl.multiple_of(blocks_ref[0, i] * LANES, LANES)
        t = pl.multiple_of(blocks_ref[1, i] * LANES, LANES)
        acc = jnp.zeros((LANES, LANES), jnp.float32)
        for k in range(0, depth, chunk):
            acc += nt(scratch[pl.ds(p, LANES), k : k + chunk], scratch[pl.ds(t, LANES), k : k + chunk])
        store(pl.ds(pl.multiple_of(i * LANES, LANES), LANES), acc)
        return 0

    lax.fori_loop(0, count, block, 0)

    def cross(i, _):
        at = pl.ds(pl.multiple_of((base_ref[0] + i) * LANES, LANES), LANES)
        acc = jnp.zeros((width, LANES), jnp.float32)
        for k in range(0, depth, chunk):
            acc += nt(applied_ref[:, lo + k : lo + k + chunk], scratch[at, k : k + chunk])
        store(pl.ds(pl.multiple_of(count * LANES + i * width, 8), width), acc)
        return 0

    lax.fori_loop(0, (out_ref.shape[0] - count * LANES) // width, cross, 0)


def project_kernel(index_ref, inv_ref, mine_ref, other_ref, proj_ref, crosst):
    rows = proj_ref.shape[0]
    panels = crosst.shape[1] // LANES
    core = index_ref[0] & 1
    for m in range(crosst.shape[0] // rows):
        for j in range(panels):
            block = pick((mine_ref, other_ref), core, m, slice(rows * j, rows * (j + 1)))
            crosst[rows * m : rows * (m + 1), LANES * j : LANES * (j + 1)] = block
    mine = pl.ds(pl.multiple_of(index_ref[0] * rows, 8), rows)
    half = nt(inv_ref[mine, :], crosst[...])
    proj_ref[...] = nt(half, inv_ref[...])


def invert(x_ref, start, stop):
    size = x_ref.shape[0]
    n = size // LANES

    def at(t):
        return pl.ds(pl.multiple_of(t * LANES, LANES), LANES)

    def step(p, _):
        x = diag_factor(x_ref[at(p), at(p)])
        panel = mm(x, x_ref[at(p), :], HIGH)
        x_ref[at(p), :] = panel
        x_ref[at(p), at(p)] = x

        def trailing(t, _):
            coef = jnp.transpose(x_ref[at(p), at(t)])
            x_ref[at(t), at(p)] = jnp.zeros((LANES, LANES), jnp.float32)
            x_ref[at(t), :] = x_ref[at(t), :] - mm(coef, x_ref[at(p), :], HIGH)
            return 0

        lax.fori_loop(p + 1, n, trailing, 0)
        return 0

    lax.fori_loop(start, stop, step, 0)
    for t in range(n - 1 if stop == n else 0):
        x_ref[LANES * t : LANES * (t + 1), LANES * (t + 1) :] = jnp.zeros((LANES, size - LANES * (t + 1)), jnp.float32)


def spot(p, t):
    return slice(LANES * p, LANES * (p + 1)), slice(LANES * t, LANES * (t + 1))


def unpack_upper(pair, core, part, per, n, x_ref):
    i = 0
    modes = 2 * pair[0].shape[0]
    for p in range(n):
        for t in range(n):
            if t >= p:
                m, r = divmod(i, per)
                x_ref[spot(p, t)] = pick(pair, core, part * modes // 2 + m, slice(LANES * r, LANES * (r + 1)))
                i += 1
            else:
                x_ref[spot(p, t)] = jnp.zeros((LANES, LANES), jnp.float32)


def first_inverse_kernel(n, per, index_ref, mine_ref, other_ref, x_ref):
    unpack_upper((mine_ref, other_ref), index_ref[0] & 1, 0, per, n, x_ref)
    invert(x_ref, 0, 1)


def rest_inverse_kernel(n, held_ref, x_ref):
    x_ref[...] = held_ref[...]
    invert(x_ref, 1, n)


def second_inverse_kernel(n, per_own, per_across, meta, keep, index_ref, first_ref, own_mine, own_other, late_mine, late_other, *refs):
    pieces, (x_ref, ortho_ref, scratch, corner, work, sem) = refs[: len(meta)], refs[len(meta) :]
    copies = load_pieces(index_ref, keep, list(zip(meta, pieces)), 0, scratch, sem)
    core = index_ref[0] & 1
    size = n * LANES
    for p in range(n):
        for t in range(n):
            m, r = divmod(p * n + t, per_across)
            corner[spot(p, t)] = pick((late_mine, late_other), core, m, slice(LANES * r, LANES * (r + 1)))
    unpack_upper((own_mine, own_other), core, 1, per_own, n, work)
    first = first_ref[...]
    upper = mm(first, corner[...], HIGH)
    lower = jnp.transpose(upper)
    work[...] = work[...] - mm(lower, upper, HIGH)
    for p in range(n):
        for t in range(p):
            work[spot(p, t)] = jnp.zeros((LANES, LANES), jnp.float32)
    corner[...] = mm(lower, first, HIGH)
    invert(work, 0, n)
    x_ref[:size, :size] = first
    x_ref[:size, size:] = jnp.zeros((size, size), jnp.float32)
    x_ref[size:, size:] = work[...]
    x_ref[size:, :size] = -mm(work[...], corner[...], HIGH)
    rows = ortho_ref.shape[0]
    mine = pl.ds(pl.multiple_of(index_ref[0] * rows, 8), rows)
    for copy in copies:
        copy.wait()
    chunk = min(512, ortho_ref.shape[1])

    def block(i, _):
        at = pl.ds(pl.multiple_of(i * chunk, chunk), chunk)
        ortho_ref[:, at] = mm(x_ref[mine, :], scratch[:, at], HIGH)
        return 0

    lax.fori_loop(0, ortho_ref.shape[1] // chunk, block, 0)


def cost(flops, moved):
    return pl.CostEstimate(flops=int(flops), bytes_accessed=int(moved), transcendentals=0)


def share(blocks, parts, index):
    per = -(-len(blocks) // parts)
    table = jnp.array(blocks + blocks[-1:] * (per * parts - len(blocks)), jnp.int32).T
    return per, lax.dynamic_slice_in_dim(table, index * per, per, 1)


def per_device(subspace, applied):
    width, depth = subspace.shape
    modes = lax.axis_size("modes")
    size = width * modes
    total = float(depth * lax.axis_size("atoms"))
    top = modes.bit_length() - 2
    lower_bits = list(reversed(range(top)))
    n = size // 2 // LANES
    mode = lax.axis_index("modes")
    index = mode[None]
    cut = depth // 2

    near = [(0, 0, subspace)]
    far = []
    for lo, hi in ((0, cut), (cut, depth)):
        far.append([(1 << top, lo, swap(subspace[:, lo:hi], "modes", top))])
    for b in lower_bits:
        near += [(mask ^ (1 << b), lo, swap(piece, "modes", b)) for mask, lo, piece in near]
    for held in far:
        for b in lower_bits:
            held += [(mask ^ (1 << b), lo, swap(piece, "modes", b)) for mask, lo, piece in held]

    smem = pl.BlockSpec(memory_space=pltpu.SMEM)

    half_keep = modes // 2 - 1
    leading = side("modes", top) == 0
    own = [(p, t) for p in range(n) for t in range(p, n)]
    per_own, own_share = share(own, modes // 2, mode & half_keep)
    across = [(p, n + t) for p in range(n) for t in range(n)]
    per_across, across_share = share(across, modes, mode)

    def products(blocks, base, rows, keep, lo, span, pieces, sums=None):
        meta = tuple((mask, start) for mask, start, _ in pieces)
        given = [index, blocks, base, applied] + ([] if sums is None else [sums])
        return pl.pallas_call(
            functools.partial(products_kernel, meta, keep, lo, total, sums is not None),
            out_shape=jax.ShapeDtypeStruct((blocks.shape[1] * LANES + n * width, LANES), jnp.float32),
            in_specs=[smem] * 3 + [VMEM] * (len(given) - 3) + [ANY] * len(pieces),
            out_specs=VMEM,
            scratch_shapes=[pltpu.VMEM((rows, span), jnp.float32), pltpu.SemaphoreType.DMA((len(pieces),))],
            cost_estimate=cost(3e9, 4 * rows * span),
        )(*given, *[piece for _, _, piece in pieces])

    early = products(own_share, jnp.zeros((1,), jnp.int32), size // 2, half_keep, 0, depth, near)
    early = all_reduce_atoms(early)
    gram_own = gather_modes_pair(early[: per_own * LANES])

    other_base = jnp.where(leading, n, 0)[None]
    late = None
    for held in far:
        lo, span = held[0][1], held[0][2].shape[1]
        late = products(across_share, other_base, size, modes - 1, lo, span, near + held, late)
    late = all_reduce_atoms(late)
    gram_across = gather_modes_pair(late[: per_across * LANES])
    cross_own, cross_across = early[per_own * LANES :], late[per_across * LANES :]
    crosst = jnp.concatenate(
        [jnp.where(leading, cross_own, cross_across), jnp.where(leading, cross_across, cross_own)], 0
    )
    crosst = gather_modes_pair(crosst)

    first_call = pl.pallas_call(
        functools.partial(first_inverse_kernel, n, per_own),
        out_shape=jax.ShapeDtypeStruct((size // 2, size // 2), jnp.float32),
        in_specs=[smem, VMEM, VMEM],
        out_specs=VMEM,
        cost_estimate=cost(5e9, 1e6),
        name="inverse_first",
    )
    first = first_call(index, *gram_own)
    rest_call = pl.pallas_call(
        functools.partial(rest_inverse_kernel, n),
        out_shape=jax.ShapeDtypeStruct((size // 2, size // 2), jnp.float32),
        in_specs=[VMEM],
        out_specs=VMEM,
        cost_estimate=cost(10e9, 1e6),
        name="inverse_rest",
    )
    first = rest_call(first)

    pieces = near + far[0] + far[1]
    meta = tuple((mask, start) for mask, start, _ in pieces)
    second_call = pl.pallas_call(
        functools.partial(second_inverse_kernel, n, per_own, per_across, meta, modes - 1),
        out_shape=(
            jax.ShapeDtypeStruct((size, size), jnp.float32),
            jax.ShapeDtypeStruct((width, depth), jnp.float32),
        ),
        in_specs=[smem] + [VMEM] * 5 + [ANY] * len(pieces),
        out_specs=(VMEM, VMEM),
        scratch_shapes=[
            pltpu.VMEM((size, depth), jnp.float32),
            pltpu.VMEM((size // 2, size // 2), jnp.float32),
            pltpu.VMEM((size // 2, size // 2), jnp.float32),
            pltpu.SemaphoreType.DMA((len(pieces),)),
        ],
        cost_estimate=cost(20e9, 8e6),
        name="inverse_second",
    )
    inv_lower, ortho = second_call(index, first, *gram_own, *gram_across, *[piece for _, _, piece in pieces])
    projected = pl.pallas_call(
        project_kernel,
        out_shape=jax.ShapeDtypeStruct((width, size), jnp.float32),
        in_specs=[smem, VMEM, VMEM, VMEM],
        out_specs=VMEM,
        scratch_shapes=[pltpu.VMEM((size, size), jnp.float32)],
        cost_estimate=cost(2e9, 5e6),
        name="project",
    )(index, inv_lower, *crosst)
    return ortho, projected


def solution(mesh):
    return jax.shard_map(
        per_device,
        mesh=mesh,
        in_specs=(P("modes", "atoms"), P("modes", "atoms")),
        out_specs=(P("modes", "atoms"), P("modes", None)),
        check_vma=False,
    )
```

```python
import functools

import jax
import jax.numpy as jnp
from jax import lax
from jax.experimental import pallas as pl
from jax.experimental.pallas import tpu as pltpu
from jax.sharding import PartitionSpec as P


HIGH = lax.Precision.HIGH
VMEM = pl.BlockSpec(memory_space=pltpu.VMEM)
ANY = pl.BlockSpec(memory_space=pl.ANY)

LANES = 128
SUB = 32
PREC = lax.Precision.HIGHEST


def mm(a, b, prec=None):
    return lax.dot_general(a, b, (((1,), (0,)), ((), ())), precision=prec or PREC, preferred_element_type=jnp.float32)


def base_factor(w, s):
    lane = lax.broadcasted_iota(jnp.int32, (SUB, LANES), 1)
    row = lax.broadcasted_iota(jnp.int32, (SUB, LANES), 0)
    sub = lax.broadcasted_iota(jnp.int32, (8, LANES), 0)

    def column(rows, k):
        return [jnp.broadcast_to(r[:, SUB * s + k : SUB * s + k + 1], (8, LANES)) for r in rows]

    def one(tile, r):
        return jnp.broadcast_to(tile[r : r + 1], (8, LANES))

    groups = SUB // 8
    first = [w[8 * g : 8 * (g + 1)] for g in range(groups)]
    in_block = (lane >= SUB * s) & (lane < SUB * (s + 1))
    own = jnp.where(in_block, (lane - SUB * s == row).astype(jnp.float32), w)
    held = [own[8 * g : 8 * (g + 1)] for g in range(groups)]
    raw = list(first)
    ahead = SUB // 2
    cols = {m: column(first[m // 8 :], m) for m in range(ahead)}
    scales = [jnp.ones((8, LANES), jnp.float32) for _ in range(groups)]
    for k in range(SUB):
        g, r = divmod(k, 8)
        if k == 8:
            for m in range(ahead, SUB):
                cols[m] = column(raw[m // 8 :], m)
        mine = cols.pop(k)
        pivot = one(mine[0], r)
        scales[g] = jnp.where(sub == r, lax.rsqrt(pivot), scales[g])
        inv = 1.0 / pivot
        mult = [t * inv for t in mine]
        mult[0] = jnp.where(sub > r, mult[0], 0.0)
        for m, tiles in cols.items():
            across = one(mine[m // 8 - g], m % 8)
            cols[m] = [t - mult[i + m // 8 - g] * across for i, t in enumerate(tiles)]
        base = one(held[g], r)
        if k < 8:
            across = one(raw[g], r)
            for i in range(g, groups):
                raw[i] = raw[i] - mult[i - g] * across
        for i in range(g, groups):
            held[i] = held[i] - mult[i - g] * base
    return jnp.concatenate([h * c for h, c in zip(held, scales)], 0)


def diag_factor(a):
    n = LANES // SUB
    blocks = [a[SUB * t : SUB * (t + 1)] for t in range(n)]
    lane = lax.broadcasted_iota(jnp.int32, (SUB, LANES), 1)
    for s in range(n):
        blocks[s] = base_factor(blocks[s], s)
        if s + 1 < n:
            coef = jnp.transpose(blocks[s])[SUB * (s + 1) :]
            delta = mm(coef, blocks[s])
            keep = (lane < SUB * s) | (lane >= SUB * (s + 1))
            for t in range(s + 1, n):
                blocks[t] = jnp.where(keep, blocks[t], 0.0) - delta[SUB * (t - s - 1) : SUB * (t - s)]
    full = jnp.concatenate(blocks, 0)
    r = lax.broadcasted_iota(jnp.int32, (LANES, LANES), 0)
    c = lax.broadcasted_iota(jnp.int32, (LANES, LANES), 1)
    return jnp.where(c <= r, full, 0.0)


def nt(a, b, prec=HIGH):
    return lax.dot_general(a, b, (((1,), (1,)), ((), ())), precision=prec, preferred_element_type=jnp.float32)


def bits(axis):
    return range(lax.axis_size(axis).bit_length() - 1)


def swap(x, axis, bit):
    return lax.ppermute(x, axis, [(i, i ^ (1 << bit)) for i in range(lax.axis_size(axis))])


def side(axis, bit):
    return (lax.axis_index(axis) >> bit) & 1


def reduce_scatter_bit(x, axis, bit):
    half = x.shape[0] // 2
    b = side(axis, bit)
    send = lax.dynamic_slice_in_dim(x, (1 - b) * half, half, 0)
    got = swap(send, axis, bit)
    return lax.dynamic_slice_in_dim(x, b * half, half, 0) + got


def all_gather_bit(x, axis, bit):
    other = swap(x, axis, bit)
    first = side(axis, bit) == 0
    return jnp.concatenate([jnp.where(first, x, other), jnp.where(first, other, x)], 0)


def all_reduce_atoms(x):
    order = list(bits("atoms"))
    scattered = []
    for b in order:
        if b != order[-1] and x.shape[0] % 16 == 0:
            x = reduce_scatter_bit(x, "atoms", b)
            scattered.append(b)
        else:
            got = swap(x, "atoms", b)
            x = x + got
    for b in reversed(scattered):
        x = all_gather_bit(x, "atoms", b)
    return x


def gather_modes_pair(x):
    shape = x.shape
    x = x[None]
    for b in reversed(bits("modes")):
        other = swap(x, "modes", b)
        if b == 0:
            return x, other
        first = side("modes", b) == 0
        x = jnp.stack([jnp.where(first, x, other), jnp.where(first, other, x)], 1).reshape((-1,) + shape)


def pick(pair, core, mode, rows):
    mine, other = pair
    group, which = divmod(mode, 2)
    return jnp.where(core == which, mine[group, rows, :], other[group, rows, :])


def load_pieces(index_ref, keep, pieces, lo, scratch, sem):
    copies = []
    hi = lo + scratch.shape[1]
    for (mask, start), ref in pieces:
        rows = ref.shape[0]
        row = pl.multiple_of(((index_ref[0] ^ mask) & keep) * rows, 8)
        left, right = max(lo, start), min(hi, start + ref.shape[1])
        if left < right:
            source = ref.at[:, pl.ds(left - start, right - left)]
            target = scratch.at[pl.ds(row, rows), pl.ds(left - lo, right - left)]
            copies.append(pltpu.make_async_copy(source, target, sem.at[len(copies)]))
    for copy in copies:
        copy.start()
    return copies


def products_kernel(meta, keep, lo, total, with_sum, panels, index_ref, blocks_ref, base_ref, applied_ref, *refs):
    sums, refs = (refs[:1], refs[1:]) if with_sum else ((), refs)
    pieces, (out_ref, scratch, sem) = refs[: len(meta)], refs[len(meta) :]
    for copy in load_pieces(index_ref, keep, list(zip(meta, pieces)), lo, scratch, sem):
        copy.wait()
    depth = scratch.shape[1]
    chunk = min(512, depth)
    width = applied_ref.shape[0]
    count = (out_ref.shape[0] - panels * width) // LANES
    own_blocks = (index_ref[0] & keep) * count

    def store(at, acc):
        acc = acc / total
        out_ref[at, :] = acc + sums[0][at, :] if with_sum else acc

    def block(i, _):
        p = pl.multiple_of(blocks_ref[0, own_blocks + i] * LANES, LANES)
        t = pl.multiple_of(blocks_ref[1, own_blocks + i] * LANES, LANES)
        acc = jnp.zeros((LANES, LANES), jnp.float32)
        for k in range(0, depth, chunk):
            acc += nt(scratch[pl.ds(p, LANES), k : k + chunk], scratch[pl.ds(t, LANES), k : k + chunk])
        store(pl.ds(pl.multiple_of(i * LANES, LANES), LANES), acc)
        return 0

    lax.fori_loop(0, count, block, 0)

    def cross(i, _):
        at = pl.ds(pl.multiple_of((base_ref[0] + i) * LANES, LANES), LANES)
        acc = jnp.zeros((width, LANES), jnp.float32)
        for k in range(0, depth, chunk):
            acc += nt(applied_ref[:, lo + k : lo + k + chunk], scratch[at, k : k + chunk])
        store(pl.ds(pl.multiple_of(count * LANES + i * width, 8), width), acc)
        return 0

    lax.fori_loop(0, panels, cross, 0)


def project_kernel(index_ref, inv_ref, mine_ref, other_ref, proj_ref, crosst):
    rows = proj_ref.shape[0]
    panels = crosst.shape[1] // LANES
    core = index_ref[0] & 1
    for m in range(crosst.shape[0] // rows):
        for j in range(panels):
            block = pick((mine_ref, other_ref), core, m, slice(rows * j, rows * (j + 1)))
            crosst[rows * m : rows * (m + 1), LANES * j : LANES * (j + 1)] = block
    mine = pl.ds(pl.multiple_of(index_ref[0] * rows, 8), rows)
    half = nt(inv_ref[mine, :], crosst[...])
    proj_ref[...] = nt(half, inv_ref[...])


def invert(x_ref, start, stop):
    size = x_ref.shape[0]
    n = size // LANES

    def at(t):
        return pl.ds(pl.multiple_of(t * LANES, LANES), LANES)

    def step(p, _):
        x = diag_factor(x_ref[at(p), at(p)])
        panel = mm(x, x_ref[at(p), :], HIGH)
        x_ref[at(p), :] = panel
        x_ref[at(p), at(p)] = x

        def trailing(t, _):
            coef = jnp.transpose(x_ref[at(p), at(t)])
            x_ref[at(t), at(p)] = jnp.zeros((LANES, LANES), jnp.float32)
            x_ref[at(t), :] = x_ref[at(t), :] - mm(coef, x_ref[at(p), :], HIGH)
            return 0

        lax.fori_loop(p + 1, n, trailing, 0)
        return 0

    lax.fori_loop(start, stop, step, 0)
    for t in range(n - 1 if stop == n else 0):
        x_ref[LANES * t : LANES * (t + 1), LANES * (t + 1) :] = jnp.zeros((LANES, size - LANES * (t + 1)), jnp.float32)


def spot(p, t):
    return slice(LANES * p, LANES * (p + 1)), slice(LANES * t, LANES * (t + 1))


def unpack_upper(pair, core, part, per, n, x_ref):
    i = 0
    modes = 2 * pair[0].shape[0]
    for p in range(n):
        for t in range(n):
            if t >= p:
                m, r = divmod(i, per)
                x_ref[spot(p, t)] = pick(pair, core, part * modes // 2 + m, slice(LANES * r, LANES * (r + 1)))
                i += 1
            else:
                x_ref[spot(p, t)] = jnp.zeros((LANES, LANES), jnp.float32)


def first_inverse_kernel(n, per, index_ref, mine_ref, other_ref, x_ref):
    unpack_upper((mine_ref, other_ref), index_ref[0] & 1, 0, per, n, x_ref)
    invert(x_ref, 0, 1)


def rest_inverse_kernel(n, held_ref, x_ref):
    x_ref[...] = held_ref[...]
    invert(x_ref, 1, n)


def second_inverse_kernel(n, per_own, per_across, meta, keep, index_ref, first_ref, own_mine, own_other, late_mine, late_other, *refs):
    pieces, (x_ref, ortho_ref, scratch, corner, work, sem) = refs[: len(meta)], refs[len(meta) :]
    copies = load_pieces(index_ref, keep, list(zip(meta, pieces)), 0, scratch, sem)
    core = index_ref[0] & 1
    size = n * LANES
    for p in range(n):
        for t in range(n):
            m, r = divmod(p * n + t, per_across)
            corner[spot(p, t)] = pick((late_mine, late_other), core, m, slice(LANES * r, LANES * (r + 1)))
    unpack_upper((own_mine, own_other), core, 1, per_own, n, work)
    first = first_ref[...]
    upper = mm(first, corner[...], HIGH)
    lower = jnp.transpose(upper)
    work[...] = work[...] - mm(lower, upper, HIGH)
    for p in range(n):
        for t in range(p):
            work[spot(p, t)] = jnp.zeros((LANES, LANES), jnp.float32)
    corner[...] = mm(lower, first, HIGH)
    invert(work, 0, n)
    x_ref[:size, :size] = first
    x_ref[:size, size:] = jnp.zeros((size, size), jnp.float32)
    x_ref[size:, size:] = work[...]
    x_ref[size:, :size] = -mm(work[...], corner[...], HIGH)
    rows = ortho_ref.shape[0]
    mine = pl.ds(pl.multiple_of(index_ref[0] * rows, 8), rows)
    for copy in copies:
        copy.wait()
    chunk = min(512, ortho_ref.shape[1])

    def block(i, _):
        at = pl.ds(pl.multiple_of(i * chunk, chunk), chunk)
        ortho_ref[:, at] = mm(x_ref[mine, :], scratch[:, at], HIGH)
        return 0

    lax.fori_loop(0, ortho_ref.shape[1] // chunk, block, 0)


def cost(flops, moved):
    return pl.CostEstimate(flops=int(flops), bytes_accessed=int(moved), transcendentals=0)


def share(blocks, parts):
    per = -(-len(blocks) // parts)
    table = jnp.array(blocks + blocks[-1:] * (per * parts - len(blocks)), jnp.int32).T
    return per, table


def per_device(subspace, applied):
    width, depth = subspace.shape
    modes = lax.axis_size("modes")
    size = width * modes
    total = float(depth * lax.axis_size("atoms"))
    top = modes.bit_length() - 2
    lower_bits = list(reversed(range(top)))
    n = size // 2 // LANES
    mode = lax.axis_index("modes")
    index = mode[None]
    cut = depth * 3 // 4

    near = [(0, 0, subspace)]
    far = []
    for lo, hi in ((0, cut), (cut, depth)):
        far.append([(1 << top, lo, swap(subspace[:, lo:hi], "modes", top))])
    for b in lower_bits:
        near += [(mask ^ (1 << b), lo, swap(piece, "modes", b)) for mask, lo, piece in near]
    for held in far:
        for b in lower_bits:
            held += [(mask ^ (1 << b), lo, swap(piece, "modes", b)) for mask, lo, piece in held]

    smem = pl.BlockSpec(memory_space=pltpu.SMEM)

    half_keep = modes // 2 - 1
    leading = side("modes", top) == 0
    own = [(p, t) for p in range(n) for t in range(p, n)]
    per_own, own_share = share(own, modes // 2)
    across = [(p, n + t) for p in range(n) for t in range(n)]
    per_across, across_share = share(across, modes)

    def products(per, blocks, base, rows, keep, lo, span, pieces, sums=None):
        meta = tuple((mask, start) for mask, start, _ in pieces)
        given = [index, blocks, base, applied] + ([] if sums is None else [sums])
        return pl.pallas_call(
            functools.partial(products_kernel, meta, keep, lo, total, sums is not None, n),
            out_shape=jax.ShapeDtypeStruct((per * LANES + n * width, LANES), jnp.float32),
            in_specs=[smem] * 3 + [VMEM] * (len(given) - 3) + [ANY] * len(pieces),
            out_specs=VMEM,
            scratch_shapes=[pltpu.VMEM((rows, span), jnp.float32), pltpu.SemaphoreType.DMA((len(pieces),))],
            cost_estimate=cost(3e9, 4 * rows * span),
        )(*given, *[piece for _, _, piece in pieces])

    early = products(per_own, own_share, jnp.zeros((1,), jnp.int32), size // 2, half_keep, 0, depth, near)
    early = all_reduce_atoms(early)
    gram_own = gather_modes_pair(early[: per_own * LANES])

    other_base = jnp.where(leading, n, 0)[None]
    late = None
    for held in far:
        lo, span = held[0][1], held[0][2].shape[1]
        late = products(per_across, across_share, other_base, size, modes - 1, lo, span, near + held, late)
    late = all_reduce_atoms(late)
    gram_across = gather_modes_pair(late[: per_across * LANES])
    cross_own, cross_across = early[per_own * LANES :], late[per_across * LANES :]
    crosst = jnp.concatenate(
        [jnp.where(leading, cross_own, cross_across), jnp.where(leading, cross_across, cross_own)], 0
    )
    crosst = gather_modes_pair(crosst)

    first_call = pl.pallas_call(
        functools.partial(first_inverse_kernel, n, per_own),
        out_shape=jax.ShapeDtypeStruct((size // 2, size // 2), jnp.float32),
        in_specs=[smem, VMEM, VMEM],
        out_specs=VMEM,
        cost_estimate=cost(5e9, 1e6),
        name="inverse_first",
    )
    first = first_call(index, *gram_own)
    rest_call = pl.pallas_call(
        functools.partial(rest_inverse_kernel, n),
        out_shape=jax.ShapeDtypeStruct((size // 2, size // 2), jnp.float32),
        in_specs=[VMEM],
        out_specs=VMEM,
        cost_estimate=cost(10e9, 1e6),
        name="inverse_rest",
    )
    first = rest_call(first)

    pieces = near + far[0] + far[1]
    meta = tuple((mask, start) for mask, start, _ in pieces)
    second_call = pl.pallas_call(
        functools.partial(second_inverse_kernel, n, per_own, per_across, meta, modes - 1),
        out_shape=(
            jax.ShapeDtypeStruct((size, size), jnp.float32),
            jax.ShapeDtypeStruct((width, depth), jnp.float32),
        ),
        in_specs=[smem] + [VMEM] * 5 + [ANY] * len(pieces),
        out_specs=(VMEM, VMEM),
        scratch_shapes=[
            pltpu.VMEM((size, depth), jnp.float32),
            pltpu.VMEM((size // 2, size // 2), jnp.float32),
            pltpu.VMEM((size // 2, size // 2), jnp.float32),
            pltpu.SemaphoreType.DMA((len(pieces),)),
        ],
        cost_estimate=cost(20e9, 8e6),
        name="inverse_second",
    )
    inv_lower, ortho = second_call(index, first, *gram_own, *gram_across, *[piece for _, _, piece in pieces])
    projected = pl.pallas_call(
        project_kernel,
        out_shape=jax.ShapeDtypeStruct((width, size), jnp.float32),
        in_specs=[smem, VMEM, VMEM, VMEM],
        out_specs=VMEM,
        scratch_shapes=[pltpu.VMEM((size, size), jnp.float32)],
        cost_estimate=cost(2e9, 5e6),
        name="project",
    )(index, inv_lower, *crosst)
    return ortho, projected


def solution(mesh):
    return jax.shard_map(
        per_device,
        mesh=mesh,
        in_specs=(P("modes", "atoms"), P("modes", "atoms")),
        out_specs=(P("modes", "atoms"), P("modes", None)),
        check_vma=False,
    )
```
